32 devices in a mesh: parts: 2 (over y), section: 4 (over x, core), tile: 4 (over z).
Axes of the slice: x: 2, y: 2, z: 4, core: 2. Of those that a mesh axis runs over, the one named last changes fastest.
Arguments:
- frames: bfloat16 [8, 4, 16, 16, 128], P('parts', 'tile'), parts along dimension 0, may hold values from -8 to 8
- cache: bfloat16 [4, 4, 4, 16, 16, 128], P('section', 'parts', 'tile'), parts along dimension 1, may hold values from -4 to 4
- conv_weight: bfloat16 [4, 3, 3, 3, 128, 128], P('section'), may hold values from -0.109375 to 0.109375
- conv_bias: float32 [4, 128], P('section'), may hold values from -2 to 2
- norm_gain: float32 [4, 128], P('section'), may hold values from 0.1 to 1.9
- norm_bias: float32 [4, 128], P('section'), may hold values from -2 to 2
Outputs:
- section_outputs: bfloat16 [4, 8, 4, 16, 16, 128], P('section', 'parts', 'tile'), parts along dimension 1
The draws below stay inside these ranges and needn't reach their ends.
There are 2 independent parts, one for each index of `parts`. The reference program is written for one: setup_inputs(seed, part) draws one part's arguments, and reference() takes and returns one part's arrays. A program takes and returns all parts, laid end to end along the dimension named above; an argument that names none is the same for every part. Nothing has to cross between parts.
All inputs are finite; a program needn't handle non-finite values.
Results may differ from the reference program's by a relative error of at most 0.0056.
Values may be sent and summed in bfloat16 or wider, within the bound.
A program may use at most 64 MiB of HBM per device.

```python
import jax
import jax.numpy as jnp
from jax import lax

C = 128
GROUPS = 32
F = 4
TH = 16
TW = 16
CTX = 2
GX = 2
GY = 2
N_SECTION = 4
N_TILE = 4


def draw_frames(key, part):
    first, second, third = jax.random.split(jax.random.fold_in(key, 11), 3)
    shape = (F, N_TILE, TH, TW, C)
    position = jnp.arange(N_TILE, dtype=jnp.float32) / max(N_TILE - 1, 1)
    base = jax.random.normal(first, shape, jnp.float32)
    rise = jnp.exp(jnp.log(3.0) * position)
    pixel = jnp.exp(jax.random.uniform(second, (F, N_TILE, TH, TW, 1), jnp.float32, -0.5, 0.5))
    channel = jnp.exp(jax.random.uniform(third, (C,), jnp.float32, -1.2, 1.2))
    values = base * rise[None, :, None, None, None] * pixel * channel
    return jnp.clip(values, -8.0, 8.0).astype(jnp.bfloat16)


def block_levels(own_key, shape, shards, low, largest):
    level, own = 1.0, jax.random.fold_in(own_key, 6)
    for dim, parts in shards:
        steps = jnp.exp(jax.random.uniform(jax.random.fold_in(own, dim), (parts,), jnp.float32, low / len(shards), largest / len(shards)))
        level = level * jnp.repeat(steps, shape[dim] // parts).reshape([-1 if axis == dim else 1 for axis in range(len(shape))])
    return level


def scatter_about(own_key, dims, scale, reach, cuts=(), held_as=jnp.bfloat16):
    loudness = block_levels(own_key, dims, cuts, -0.22, 0.18) if cuts else 1.0
    drawn = jax.random.normal(own_key, dims, jnp.float32) * scale * loudness
    return jnp.minimum(jnp.maximum(drawn, -reach), reach).astype(held_as)


def setup_inputs(seed: int = 0, part: int = 0) -> dict:
    key_of = jax.random.split(jax.random.key(seed), 7)
    part_keys = jax.random.split(jax.random.fold_in(key_of[6], part), 7)
    return {
        "frames": draw_frames(jax.random.fold_in(jax.random.fold_in(key_of[6], part), 71), part),
        "cache": scatter_about(part_keys[1], (N_SECTION, CTX, N_TILE, TH, TW, C), 0.6, 4.0, ((0, 4), (2, 4))),
        "conv_weight": scatter_about(key_of[2], (N_SECTION, 3, 3, 3, C, C), (27 * C) ** -0.5, 0.109375, ((0, 4),)),
        "conv_bias": scatter_about(key_of[3], (N_SECTION, C), 0.3, 2.0, ((0, 4),), jnp.float32),
        "norm_gain": jnp.clip(1.0 + 0.18 * jax.random.normal(key_of[4], (N_SECTION, C), jnp.float32), 0.1, 1.9),
        "norm_bias": scatter_about(key_of[5], (N_SECTION, C), 0.3, 2.0, ((0, 4),), jnp.float32),
    }


EPSILON = 1e-06

def to_image(tiles):
    count = tiles.shape[0]
    placed = jnp.roll(tiles, GX + 2, axis=1)
    grid = placed.reshape(count, GY, GX, TH, TW, C)
    return grid.transpose(0, 1, 3, 2, 4, 5).reshape(count, GY * TH, GX * TW, C)

def to_tiles(image):
    count = image.shape[0]
    grid = image.reshape(count, GY, TH, GX, TW, C)
    placed = grid.transpose(0, 1, 3, 2, 4, 5).reshape(count, GY * GX, TH, TW, C)
    return jnp.roll(placed, -(GX + 2), axis=1)

def reference(frames, cache, conv_weight, conv_bias, norm_gain, norm_bias):
    state = to_image(frames)
    height = GY * TH
    width = GX * TW
    results = []
    for section in range(N_SECTION):
        values = state.astype(jnp.float32)
        grouped = values.reshape(F, height * width, GROUPS, C // GROUPS)
        mean = lax.optimization_barrier(jnp.mean(grouped, axis=(1, 3), keepdims=True))
        centered = grouped - mean
        variance = lax.optimization_barrier(jnp.mean(centered * centered, axis=(1, 3), keepdims=True))
        normed = (centered / jnp.sqrt(variance + EPSILON)).reshape(F, height, width, C)
        normed = normed * norm_gain[section] + norm_bias[section]
        active = jax.nn.silu(normed).astype(jnp.bfloat16)
        sequence = jnp.concatenate([to_image(cache[section]), active], axis=0)
        padded = jnp.pad(sequence, ((0, 0), (1, 1), (1, 1), (0, 0)))
        total = jnp.zeros((F * height * width, C), jnp.float32)
        for step_t in range(3):
            for step_y in range(3):
                for step_x in range(3):
                    window = padded[step_t:step_t + F, step_y:step_y + height, step_x:step_x + width]
                    total = total + jnp.dot(window.reshape(F * height * width, C), conv_weight[section, step_t, step_y, step_x], preferred_element_type=jnp.float32)
        total = total.reshape(F, height, width, C)
        state = (values + total + conv_bias[section]).astype(jnp.bfloat16)
        results.append(to_tiles(state))
    return jnp.stack(results)
```

```python
import functools

import jax
import jax.numpy as jnp
from jax import lax
from jax.experimental import pallas as pl
from jax.experimental.pallas import tpu as pltpu
from jax.sharding import PartitionSpec as P

GROUPS = 32
EPSILON = 1e-06
EDGE = 8
STATS = 8


def kernel(
    sections, tiles, height, width,
    frames_ref, cache_ref, weight_ref, bias_ref, gain_ref, offset_ref, out_ref,
    weight, main, outgoing, notes, drafts, old_notes, old_drafts, totals, wide, patches, state,
    weight_sem, main_sem, main_sent, note_sem, note_sent, first_sent, old_sem, old_sent,
):
    count, pixels, channels = frames_ref.shape
    context = cache_ref.shape[0]
    taps = weight_ref.shape[0] // (3 * channels * 3)
    halo = max(height, width)
    pitch = width + 2 * EDGE
    section = lax.axis_index("section")
    tile = lax.axis_index("tile")
    across = min(8, tiles // 2)
    down = tiles // across
    shift = across + 2

    def spot(index):
        image = lax.rem(index + shift, tiles)
        return image // across, lax.rem(image, across)

    row, column = spot(tile)

    def at_tile(peer_row, peer_column):
        return lax.rem(peer_row * across + peer_column + 2 * tiles - shift, tiles)

    def direction(peer):
        peer_row, peer_column = spot(peer)
        dy, dx = peer_row - row, peer_column - column
        near = (dy >= -1) & (dy <= 1) & (dx >= -1) & (dx <= 1)
        return jnp.where(near, (dy + 1) * 3 + dx + 1, 4)

    peers = [lax.rem(tile + step, tiles) for step in range(1, tiles)]
    last = section == sections - 1
    barrier = pltpu.get_barrier_semaphore()

    for peer in peers:
        pl.semaphore_signal(
            barrier, inc=1, device_id={"section": section, "tile": peer}, device_id_type=pl.DeviceIdType.MESH
        )

    @pl.when(section > 0)
    def _():
        for peer in peers + [tile]:
            pl.semaphore_signal(
                barrier, inc=1, device_id={"section": section - 1, "tile": peer},
                device_id_type=pl.DeviceIdType.MESH,
            )

    fetch = pltpu.make_async_copy(weight_ref, weight, weight_sem)
    fetch.start()

    def borders(target, values, stats):
        state[...] = values
        top, bottom = values[:width], values[pixels - width :]
        left = state[pl.ds(0, height, stride=width), :]
        right = state[pl.ds(width - 1, height, stride=width), :]
        pieces = [
            values[:width], top, values[:width],
            left, None, right,
            bottom, bottom, bottom,
        ]
        for place, piece in enumerate(pieces):
            if piece is not None:
                target[place, : piece.shape[0], :] = piece
            if stats is not None:
                target[place, halo : halo + STATS, :] = stats

    def measure_of(values):
        total = jnp.sum(values, axis=0, keepdims=True)
        squares = jnp.sum(values * values, axis=0, keepdims=True)
        line = lax.broadcasted_iota(jnp.int32, (STATS, channels), 0)
        return jnp.where(line == 0, total, jnp.where(line == 1, squares, 0.0))

    def post(source, frame, section_to, sent, peer):
        pltpu.make_async_remote_copy(
            src_ref=source.at[direction(peer)],
            dst_ref=notes.at[frame, tile],
            send_sem=sent.at[frame],
            recv_sem=note_sem.at[frame],
            device_id={"section": section_to, "tile": peer},
            device_id_type=pl.DeviceIdType.MESH,
        ).start()

    for frame in range(context):
        borders(old_drafts.at[frame], cache_ref[frame].astype(jnp.float32), None)

    @pl.when(section == 0)
    def _():
        for frame in range(count):
            values = frames_ref[frame].astype(jnp.float32)
            borders(drafts.at[count + frame], values, measure_of(values))

    pl.semaphore_wait(barrier, jnp.where(last, tiles - 1, 2 * tiles - 1))

    @pl.when(section == 0)
    def _():
        for frame in range(count):
            for peer in peers:
                post(drafts.at[count + frame], frame, 0, first_sent, peer)
            pltpu.make_async_copy(
                drafts.at[count + frame, 4], notes.at[frame, tile], note_sem.at[frame]
            ).start()

    for frame in range(context):
        for peer in peers:
            pltpu.make_async_remote_copy(
                src_ref=old_drafts.at[frame, direction(peer)],
                dst_ref=old_notes.at[frame, tile],
                send_sem=old_sent.at[frame],
                recv_sem=old_sem.at[frame],
                device_id={"section": section, "tile": peer},
                device_id_type=pl.DeviceIdType.MESH,
            ).start()

    around = {}
    for dy in (-1, 0, 1):
        for dx in (-1, 0, 1):
            if dy or dx:
                y, x = row + dy, column + dx
                inside = (y >= 0) & (y < down) & (x >= 0) & (x < across)
                around[dy, dx] = inside, jnp.where(inside, at_tile(y, x), peers[0])

    def lay_out(values, message, act):
        centre = act(values)

        def border(place, lines):
            inside, sender = around[place]
            piece = message(sender)[:lines]
            return jnp.where(inside, act(piece), 0.0)

        for y in range(height):
            wide[(1 + y) * pitch + EDGE : (1 + y) * pitch + EDGE + width, :] = centre[
                y * width : (y + 1) * width
            ]
        for dy, line in ((-1, 0), (1, height + 1)):
            base = line * pitch + EDGE
            wide[base : base + width, :] = border((dy, 0), width)
        for dx, spot_x in ((-1, EDGE - 1), (1, EDGE + width)):
            wide[pl.ds(pitch + spot_x, height, stride=pitch), :] = border((0, dx), height)
            for dy, line in ((-1, 0), (1, height + 1)):
                inside, sender = around[dy, dx]
                where_x = 0 if dx == 1 else width - 1
                piece = act(message(sender)[where_x : where_x + 1])
                wide[line * pitch + spot_x : line * pitch + spot_x + 1, :] = jnp.where(inside, piece, 0.0)
        for line in range(height + 2):
            for dx in range(3):
                start = line * pitch + EDGE - 1 + dx
                patches[line * width : (line + 1) * width, dx * channels : (dx + 1) * channels] = wide[
                    start : start + width, :
                ].astype(jnp.bfloat16)

    def convolved(*times):
        result = None
        for dy in range(3):
            kernels = [
                weight[(t * 3 + dy) * 3 * channels : (t * 3 + dy + 1) * 3 * channels, :] for t in times
            ]
            kernels = kernels[0] if len(kernels) == 1 else jnp.concatenate(kernels, axis=1)
            part = jnp.dot(
                patches[dy * width : dy * width + pixels, :], kernels, preferred_element_type=jnp.float32
            )
            result = part if result is None else result + part
        return result

    fetch.wait()
    fresh = set()

    def add(frame, value):
        if frame in fresh:
            totals[frame] += value
        else:
            totals[frame] = value
            fresh.add(frame)

    for old in range(context):
        pltpu.make_async_copy(
            old_notes.at[old, 0 : tiles - 1], old_notes.at[old, 0 : tiles - 1], old_sem.at[old]
        ).wait()
        lay_out(cache_ref[old].astype(jnp.float32), lambda sender: old_notes[old, sender], lambda v: v)
        reach = [t for t in range(taps) if 0 <= old - t < count]
        if reach:
            both = convolved(*reach)
            for at, t in enumerate(reach):
                add(old - t, both[:, at * channels : (at + 1) * channels])

    bias, gain, offset = bias_ref[...], gain_ref[...], offset_ref[...]
    members = pixels * tiles * (channels // GROUPS)
    lane = lax.broadcasted_iota(jnp.int32, (STATS, channels), 1)

    for frame in range(count):
        pltpu.make_async_copy(notes.at[frame], notes.at[frame], note_sem.at[frame]).wait()
        sums = notes[frame, 0, halo : halo + STATS]
        for sender in range(1, tiles):
            sums = sums + notes[frame, sender, halo : halo + STATS]
        step = 1
        while step < channels // GROUPS:
            sums = sums + jnp.where(
                (lane // step) % 2 == 0,
                pltpu.roll(sums, channels - step, 1),
                pltpu.roll(sums, step, 1),
            )
            step *= 2
        mean = sums[0:1] / members
        variance = jnp.maximum(sums[1:2] / members - mean * mean, 0.0)
        scale = gain / jnp.sqrt(variance + EPSILON)

        def act(values):
            value = (values - mean) * scale + offset
            return value / (1.0 + jnp.exp(-value))

        @pl.when(section > 0)
        def _():
            pltpu.make_async_copy(main.at[frame], main.at[frame], main_sem.at[frame]).wait()

        @pl.when(section == 0)
        def _():
            main[frame] = frames_ref[frame]

        values = main[frame].astype(jnp.float32)
        lay_out(values, lambda sender: notes[frame, sender], act)
        result = values + bias + convolved(taps - 1)
        if frame in fresh:
            result = result + totals[frame]
        rounded = result.astype(jnp.bfloat16)
        out_ref[frame] = rounded

        @pl.when(jnp.logical_not(last))
        def _():
            outgoing[frame] = rounded
            pltpu.make_async_remote_copy(
                src_ref=outgoing.at[frame],
                dst_ref=main.at[frame],
                send_sem=main_sent.at[frame],
                recv_sem=main_sem.at[frame],
                device_id={"section": section + 1, "tile": tile},
                device_id_type=pl.DeviceIdType.MESH,
            ).start()
            kept = rounded.astype(jnp.float32)
            borders(drafts.at[frame], kept, measure_of(kept))
            for peer in peers + [tile]:
                post(drafts.at[frame], frame, section + 1, note_sent, peer)

        reach = [t for t in range(taps - 1) if context + frame - t < count]
        if reach:
            both = convolved(*reach)
            for at, t in enumerate(reach):
                add(context + frame - t, both[:, at * channels : (at + 1) * channels])

    for frame in range(context):
        pltpu.make_async_copy(
            old_notes.at[frame, 0 : tiles - 1], old_notes.at[frame, 0 : tiles - 1], old_sent.at[frame]
        ).wait()

    for frame in range(count):
        @pl.when(section == 0)
        def _():
            pltpu.make_async_copy(
                notes.at[frame, 0 : tiles - 1], notes.at[frame, 0 : tiles - 1], first_sent.at[frame]
            ).wait()

        @pl.when(jnp.logical_not(last))
        def _():
            pltpu.make_async_copy(outgoing.at[frame], outgoing.at[frame], main_sent.at[frame]).wait()
            pltpu.make_async_copy(notes.at[frame], notes.at[frame], note_sent.at[frame]).wait()


def local(frames, cache, conv_weight, conv_bias, norm_gain, norm_bias):
    sections = lax.axis_size("section")
    tiles = lax.axis_size("tile")
    count, _, height, width, channels = frames.shape
    context = cache.shape[1]
    pixels = height * width
    lines = max(height, width)
    pitch = width + 2 * EDGE
    vmem = pl.BlockSpec(memory_space=pltpu.VMEM)
    dma = pltpu.SemaphoreType.DMA
    result = pl.pallas_call(
        functools.partial(kernel, sections, tiles, height, width),
        out_shape=jax.ShapeDtypeStruct((count, pixels, channels), jnp.bfloat16),
        in_specs=[vmem, vmem, pl.BlockSpec(memory_space=pl.ANY), vmem, vmem, vmem],
        out_specs=vmem,
        scratch_shapes=[
            pltpu.VMEM((27 * channels, channels), jnp.bfloat16),
            pltpu.VMEM((count, pixels, channels), jnp.bfloat16),
            pltpu.VMEM((count, pixels, channels), jnp.bfloat16),
            pltpu.VMEM((count, tiles, lines + STATS, channels), jnp.float32),
            pltpu.VMEM((2 * count, 9, lines + STATS, channels), jnp.float32),
            pltpu.VMEM((context, tiles, lines, channels), jnp.float32),
            pltpu.VMEM((context, 9, lines, channels), jnp.float32),
            pltpu.VMEM((count, pixels, channels), jnp.float32),
            pltpu.VMEM(((height + 2) * pitch, channels), jnp.float32),
            pltpu.VMEM(((height + 2) * width, 3 * channels), jnp.bfloat16),
            pltpu.VMEM((pixels, channels), jnp.float32),
            dma,
            dma((count,)),
            dma((count,)),
            dma((count,)),
            dma((count,)),
            dma((count,)),
            dma((context,)),
            dma((context,)),
        ],
        compiler_params=pltpu.CompilerParams(collective_id=0, has_side_effects=True),
    )(
        frames.reshape(count, pixels, channels),
        cache.reshape(context, pixels, channels),
        conv_weight.reshape(27 * channels, channels),
        conv_bias,
        norm_gain,
        norm_bias,
    )
    return result.reshape(1, count, 1, height, width, channels)


def solution(mesh):
    placed = (
        P("parts", "tile", None, None, None),
        P("section", "parts", "tile", None, None, None),
        P("section", None, None, None, None, None),
        P("section", None),
        P("section", None),
        P("section", None),
    )
    return jax.shard_map(
        local,
        mesh=mesh,
        in_specs=placed,
        out_specs=P("section", "parts", "tile", None, None, None),
        check_vma=False,
    )
```

```python
import functools

import jax
import jax.numpy as jnp
from jax import lax
from jax.experimental import pallas as pl
from jax.experimental.pallas import tpu as pltpu
from jax.sharding import PartitionSpec as P

GROUPS = 32
EPSILON = 1e-06
EDGE = 8


SIDES = ((-1, 0), (0, -1), (0, 1), (1, 0))
CORNERS = ((-1, -1), (-1, 1), (1, -1), (1, 1))


def kernel(
    sections, tiles, height, width,
    frames_hbm, cache_hbm, weight_hbm, bias_ref, gain_ref, offset_ref, out_ref,
    weight, main, history, outgoing, notes, drafts, sides, columns,
    old_sides, old_columns, old_corners, old_drafts, totals, wide, patches, state,
    weight_sem, main_sem, main_sent, history_sem, note_sem, note_sent, first_sent,
    side_sem, side_sent, first_side_sent, old_sem, old_sent, corner_sem, corner_sent,
):
    count, pixels, channels = main.shape
    context = history.shape[0]
    taps = weight.shape[0] // (9 * channels)
    pitch = width + 2 * EDGE
    section = lax.axis_index("section")
    tile = lax.axis_index("tile")
    across = min(8, tiles // 2)
    down = tiles // across
    shift = across + 2
    mesh_id = pl.DeviceIdType.MESH
    first = section == 0
    onward = section < sections - 1
    image = lax.rem(tile + shift, tiles)
    row, column = image // across, lax.rem(image, across)
    peers = [lax.rem(tile + step, tiles) for step in range(1, tiles)]

    around = {}
    for dy, dx in SIDES + CORNERS:
        y, x = row + dy, column + dx
        inside = (y >= 0) & (y < down) & (x >= 0) & (x < across)
        there = lax.rem(y * across + x + 2 * tiles - shift, tiles)
        around[dy, dx] = inside, jnp.where(inside, there, peers[0])

    barrier = pltpu.get_barrier_semaphore()
    for peer in peers:
        pl.semaphore_signal(
            barrier, inc=1, device_id={"section": section, "tile": peer}, device_id_type=mesh_id
        )

    @pl.when(jnp.logical_not(first))
    def _():
        for peer in peers + [tile]:
            pl.semaphore_signal(
                barrier, inc=1, device_id={"section": section - 1, "tile": peer}, device_id_type=mesh_id
            )

    def fetch_frame(frame):
        return pltpu.make_async_copy(frames_hbm.at[frame], main.at[frame], main_sem.at[frame])

    fetch_weight = pltpu.make_async_copy(weight_hbm, weight, weight_sem)
    fetch_cache = [
        pltpu.make_async_copy(cache_hbm.at[old], history.at[old], history_sem.at[old])
        for old in range(context)
    ]

    @pl.when(first)
    def _():
        for frame in range(count):
            fetch_frame(frame).start()

    for fetch in fetch_cache:
        fetch.start()
    fetch_weight.start()

    def edge_columns(target, values):
        state[...] = values
        for at, x in enumerate((0, width - 1)):
            target[at] = state[pl.ds(x, height, stride=width), :].astype(jnp.bfloat16)

    def corner_of(values, dy, dx):
        at = (height - 1) * width * (dy == 1) + (width - 1) * (dx == 1)
        return values[at : at + 1]

    def write_notes(target, values):
        total = jnp.sum(values, axis=0, keepdims=True)
        squares = jnp.sum(values * values, axis=0, keepdims=True)
        for dy in (-1, 0, 1):
            for dx in (-1, 0, 1):
                place = (dy + 1) * 3 + dx + 1
                corner = corner_of(values, dy, dx)
                target[place] = jnp.concatenate([total, squares, corner, corner], axis=0)

    def post_notes(source, frame, section_to, sent, receivers):
        for peer in receivers:
            there = lax.rem(peer + shift, tiles)
            dy, dx = there // across - row, lax.rem(there, across) - column
            near = (dy >= -1) & (dy <= 1) & (dx >= -1) & (dx <= 1)
            pltpu.make_async_remote_copy(
                src_ref=source.at[jnp.where(near, (dy + 1) * 3 + dx + 1, 4)],
                dst_ref=notes.at[frame, tile],
                send_sem=sent.at[frame],
                recv_sem=note_sem.at[frame],
                device_id={"section": section_to, "tile": peer},
                device_id_type=mesh_id,
            ).start()

    def side_copies(rows, edges, landing, section_to, sent, received):
        copies = []
        for at, (dy, dx) in enumerate(SIDES):
            source = edges.at[int(dx == 1)]
            if dy:
                start = 0 if dy < 0 else pixels - width
                source = rows.at[start : start + width]
            inside, peer = around[dy, dx]
            copy = pltpu.make_async_remote_copy(
                src_ref=source,
                dst_ref=landing.at[3 - at],
                send_sem=sent.at[at],
                recv_sem=received.at[3 - at],
                device_id={"section": section_to, "tile": peer},
                device_id_type=mesh_id,
            )
            copies.append((inside, copy))
        return copies

    def each(copies, action):
        for inside, copy in copies:
            @pl.when(inside)
            def _():
                action(copy)

    def start(copy):
        copy.start()

    def departed(copy):
        copy.wait_send()

    def arrived(copies):
        for at, (_, copy) in enumerate(copies):
            inside, _ = copies[at // 4 * 4 + 3 - at % 4]

            @pl.when(inside)
            def _():
                copy.wait_recv()

    def old_copies(old):
        copies = side_copies(
            history.at[old], old_columns.at[old], old_sides.at[old], section, old_sent.at[old], old_sem.at[old]
        )
        for at, (dy, dx) in enumerate(CORNERS):
            inside, peer = around[dy, dx]
            copy = pltpu.make_async_remote_copy(
                src_ref=old_drafts.at[old, at],
                dst_ref=old_corners.at[old, 3 - at],
                send_sem=corner_sent.at[old, at],
                recv_sem=corner_sem.at[old, 3 - at],
                device_id={"section": section, "tile": peer},
                device_id_type=mesh_id,
            )
            copies.append((inside, copy))
        return copies

    def first_sides(frame):
        return side_copies(
            main.at[frame], columns.at[count + frame], sides.at[frame], section,
            first_side_sent.at[frame], side_sem.at[frame],
        )

    def next_sides(frame):
        return side_copies(
            outgoing.at[frame], columns.at[frame], sides.at[frame], section + onward.astype(jnp.int32),
            side_sent.at[frame], side_sem.at[frame],
        )

    def own_note(frame):
        return pltpu.make_async_copy(drafts.at[count + frame, 4], notes.at[frame, tile], note_sem.at[frame])

    def open_frame(frame):
        each(first_sides(frame), start)
        post_notes(drafts.at[count + frame], frame, section, first_sent, peers)
        own_note(frame).start()

    def prepare_frame(frame):
        fetch_frame(frame).wait()
        values = main[frame].astype(jnp.float32)
        edge_columns(columns.at[count + frame], values)
        write_notes(drafts.at[count + frame], values)

    @pl.when(first)
    def _():
        prepare_frame(0)

    pl.semaphore_wait(barrier, jnp.where(onward, 2 * tiles - 1, tiles - 1))

    @pl.when(first)
    def _():
        open_frame(0)

    for old in range(context):
        fetch_cache[old].wait()
        values = history[old].astype(jnp.float32)
        edge_columns(old_columns.at[old], values)
        for at, (dy, dx) in enumerate(CORNERS):
            old_drafts[old, at] = corner_of(values, dy, dx)
        each(old_copies(old), start)

    @pl.when(first)
    def _():
        for frame in range(1, count):
            prepare_frame(frame)
            open_frame(frame)

    def lay_out(values, side, corner, act):
        centre = act(values)
        for y in range(height):
            wide[(1 + y) * pitch + EDGE : (1 + y) * pitch + EDGE + width, :] = centre[
                y * width : (y + 1) * width
            ]
        for at, (dy, dx) in enumerate(SIDES):
            inside, _ = around[dy, dx]
            piece = jnp.where(inside, act(side(at).astype(jnp.float32)), 0.0)
            if dy:
                base = (0 if dy < 0 else height + 1) * pitch + EDGE
                wide[base : base + width, :] = piece
            else:
                base = pitch + (EDGE - 1 if dx < 0 else EDGE + width)
                wide[pl.ds(base, height, stride=pitch), :] = piece
        for at, (dy, dx) in enumerate(CORNERS):
            inside, sender = around[dy, dx]
            base = (0 if dy < 0 else height + 1) * pitch + (EDGE - 1 if dx < 0 else EDGE + width)
            wide[base : base + 1, :] = jnp.where(inside, act(corner(at, sender)), 0.0)
        for line in range(height + 2):
            for dx in range(3):
                at = line * pitch + EDGE - 1 + dx
                patches[line * width : (line + 1) * width, dx * channels : (dx + 1) * channels] = wide[
                    at : at + width, :
                ].astype(jnp.bfloat16)

    def convolved(*times):
        result = None
        for dy in range(3):
            kernels = [
                weight[(t * 3 + dy) * 3 * channels : (t * 3 + dy + 1) * 3 * channels, :] for t in times
            ]
            kernels = kernels[0] if len(kernels) == 1 else jnp.concatenate(kernels, axis=1)
            part = jnp.dot(
                patches[dy * width : dy * width + pixels, :], kernels, preferred_element_type=jnp.float32
            )
            result = part if result is None else result + part
        return result

    fetch_weight.wait()
    fresh = set()

    def spread(newest, times):
        reach = [t for t in times if 0 <= newest - t < count]
        if reach:
            both = convolved(*reach)
        for at, t in enumerate(reach):
            value = both[:, at * channels : (at + 1) * channels]
            if newest - t in fresh:
                totals[newest - t] += value
            else:
                totals[newest - t] = value
                fresh.add(newest - t)

    for old in range(context):
        arrived(old_copies(old))
        lay_out(
            history[old].astype(jnp.float32),
            lambda at: old_sides[old, at],
            lambda at, sender: old_corners[old, at],
            lambda values: values,
        )
        spread(old, range(taps))

    bias, gain, offset = bias_ref[...], gain_ref[...], offset_ref[...]
    members = pixels * tiles * (channels // GROUPS)
    lane = lax.broadcasted_iota(jnp.int32, (2, channels), 1)

    for frame in range(count):
        pltpu.make_async_copy(notes.at[frame], notes.at[frame], note_sem.at[frame]).wait()
        arrived(next_sides(frame))

        @pl.when(jnp.logical_not(first))
        def _():
            fetch_frame(frame).wait()

        sums = notes[frame, 0, 0:2]
        for sender in range(1, tiles):
            sums = sums + notes[frame, sender, 0:2]
        step = 1
        while step < channels // GROUPS:
            sums = sums + jnp.where(
                (lane // step) % 2 == 0,
                jnp.roll(sums, channels - step, 1),
                jnp.roll(sums, step, 1),
            )
            step *= 2
        mean = sums[0:1] / members
        variance = jnp.maximum(sums[1:2] / members - mean * mean, 0.0)
        scale = gain / jnp.sqrt(variance + EPSILON)

        def act(values):
            value = (values - mean) * scale + offset
            return value / (1.0 + jnp.exp(-value))

        values = main[frame].astype(jnp.float32)
        lay_out(
            values, lambda at: sides[frame, at], lambda at, sender: notes[frame, sender, 2:3], act
        )
        result = values + bias + convolved(taps - 1)
        if frame in fresh:
            result = result + totals[frame]
        rounded = result.astype(jnp.bfloat16)
        out_ref[frame] = rounded

        @pl.when(onward)
        def _():
            outgoing[frame] = rounded
            pltpu.make_async_remote_copy(
                src_ref=outgoing.at[frame],
                dst_ref=main.at[frame],
                send_sem=main_sent.at[frame],
                recv_sem=main_sem.at[frame],
                device_id={"section": section + 1, "tile": tile},
                device_id_type=mesh_id,
            ).start()
            kept = rounded.astype(jnp.float32)
            write_notes(drafts.at[frame], kept)
            post_notes(drafts.at[frame], frame, section + 1, note_sent, peers + [tile])
            edge_columns(columns.at[frame], kept)
            each(next_sides(frame), start)

        spread(context + frame, range(taps - 1))

    for old in range(context):
        each(old_copies(old), departed)

    @pl.when(first)
    def _():
        for frame in range(count):
            each(first_sides(frame), departed)
            some = notes.at[frame, 0 : tiles - 1]
            pltpu.make_async_copy(some, some, first_sent.at[frame]).wait()

    @pl.when(onward)
    def _():
        for frame in range(count):
            pltpu.make_async_copy(outgoing.at[frame], outgoing.at[frame], main_sent.at[frame]).wait()
            pltpu.make_async_copy(notes.at[frame], notes.at[frame], note_sent.at[frame]).wait()
            each(next_sides(frame), departed)


def local(frames, cache, conv_weight, conv_bias, norm_gain, norm_bias):
    sections = lax.axis_size("section")
    tiles = lax.axis_size("tile")
    count, _, height, width, channels = frames.shape
    context = cache.shape[1]
    pixels = height * width
    pitch = width + 2 * EDGE
    rows = conv_weight.size // channels
    vmem = pl.BlockSpec(memory_space=pltpu.VMEM)
    anywhere = pl.BlockSpec(memory_space=pl.ANY)
    dma = pltpu.SemaphoreType.DMA
    half, full = jnp.bfloat16, jnp.float32
    result = pl.pallas_call(
        functools.partial(kernel, sections, tiles, height, width),
        out_shape=pltpu.VMEM((count, pixels, channels), jnp.bfloat16),
        in_specs=[anywhere, anywhere, anywhere, vmem, vmem, vmem],
        out_specs=vmem,
        scratch_shapes=[
            pltpu.VMEM((rows, channels), half),
            pltpu.VMEM((count, pixels, channels), half),
            pltpu.VMEM((context, pixels, channels), half),
            pltpu.VMEM((count, pixels, channels), half),
            pltpu.VMEM((count, tiles, 4, channels), full),
            pltpu.VMEM((2 * count, 9, 4, channels), full),
            pltpu.VMEM((count, 4, width, channels), half),
            pltpu.VMEM((2 * count, 2, height, channels), half),
            pltpu.VMEM((context, 4, width, channels), half),
            pltpu.VMEM((context, 2, height, channels), half),
            pltpu.VMEM((context, 4, 1, channels), full),
            pltpu.VMEM((context, 4, 1, channels), full),
            pltpu.VMEM((count, pixels, channels), full),
            pltpu.VMEM(((height + 2) * pitch, channels), full),
            pltpu.VMEM(((height + 2) * width, 3 * channels), half),
            pltpu.VMEM((pixels, channels), full),
            dma,
            dma((count,)),
            dma((count,)),
            dma((context,)),
            dma((count,)),
            dma((count,)),
            dma((count,)),
            dma((count, 4)),
            dma((count, 4)),
            dma((count, 4)),
            dma((context, 4)),
            dma((context, 4)),
            dma((context, 4)),
            dma((context, 4)),
        ],
        compiler_params=pltpu.CompilerParams(collective_id=0, has_side_effects=True),
    )(
        frames.reshape(count, pixels, channels),
        cache.reshape(context, pixels, channels),
        conv_weight.reshape(rows, channels),
        conv_bias,
        norm_gain,
        norm_bias,
    )
    return result.reshape(1, count, 1, height, width, channels)


def solution(mesh):
    placed = (
        P("parts", "tile", None, None, None),
        P("section", "parts", "tile", None, None, None),
        P("section", None, None, None, None, None),
        P("section", None),
        P("section", None),
        P("section", None),
    )
    return jax.shard_map(
        local,
        mesh=mesh,
        in_specs=placed,
        out_specs=P("section", "parts", "tile", None, None, None),
        check_vma=False,
    )
```

```python
import functools

import jax
import jax.numpy as jnp
from jax import lax
from jax.experimental import pallas as pl
from jax.experimental.pallas import tpu as pltpu
from jax.sharding import PartitionSpec as P

GROUPS = 32
EPSILON = 1e-06
EDGE = 8


SIDES = ((-1, 0), (0, -1), (0, 1), (1, 0))
CORNERS = ((-1, -1), (-1, 1), (1, -1), (1, 1))


def kernel(
    sections, tiles, height, width,
    frames_hbm, cache_hbm, weight_hbm, bias_hbm, gain_hbm, offset_hbm, out_ref,
    weight, vectors, main, history, outgoing, notes, drafts, sides, columns,
    old_sides, old_columns, old_corners, old_drafts, totals, wide, patches, state,
    weight_sem, vector_sem, main_sem, main_sent, history_sem, note_sem, note_sent, first_sent,
    side_sem, side_sent, first_side_sent, old_sem, old_sent, corner_sem, corner_sent,
):
    count, pixels, channels = main.shape
    context = history.shape[0]
    taps = weight.shape[0] // (9 * channels)
    pitch = width + 2 * EDGE
    section = lax.axis_index("section")
    tile = lax.axis_index("tile")
    across = min(8, tiles // 2)
    down = tiles // across
    shift = across + 2
    mesh_id = pl.DeviceIdType.MESH
    first = section == 0
    onward = section < sections - 1
    image = lax.rem(tile + shift, tiles)
    row, column = image // across, lax.rem(image, across)
    peers = [lax.rem(tile + step, tiles) for step in range(1, tiles)]

    around = {}
    for dy, dx in SIDES + CORNERS:
        y, x = row + dy, column + dx
        inside = (y >= 0) & (y < down) & (x >= 0) & (x < across)
        there = lax.rem(y * across + x + 2 * tiles - shift, tiles)
        around[dy, dx] = inside, jnp.where(inside, there, peers[0])

    barrier = pltpu.get_barrier_semaphore()
    for peer in peers:
        pl.semaphore_signal(
            barrier, inc=1, device_id={"section": section, "tile": peer}, device_id_type=mesh_id
        )

    @pl.when(jnp.logical_not(first))
    def _():
        for peer in peers + [tile]:
            pl.semaphore_signal(
                barrier, inc=1, device_id={"section": section - 1, "tile": peer}, device_id_type=mesh_id
            )

    def fetch_frame(frame):
        return pltpu.make_async_copy(frames_hbm.at[frame], main.at[frame], main_sem.at[frame])

    fetch_weight = pltpu.make_async_copy(weight_hbm, weight, weight_sem)
    fetch_cache = [
        pltpu.make_async_copy(cache_hbm.at[old], history.at[old], history_sem.at[old])
        for old in range(context)
    ]

    @pl.when(first)
    def _():
        for frame in range(count):
            fetch_frame(frame).start()

    fetch_vectors = [
        pltpu.make_async_copy(source, vectors.at[at], vector_sem.at[at])
        for at, source in enumerate((bias_hbm, gain_hbm, offset_hbm))
    ]
    for fetch in fetch_cache + [fetch_weight] + fetch_vectors:
        fetch.start()

    def edge_columns(target, values):
        state[...] = values
        for at, x in enumerate((0, width - 1)):
            target[at] = state[pl.ds(x, height, stride=width), :].astype(jnp.bfloat16)

    def corner_of(values, dy, dx):
        at = (height - 1) * width * (dy == 1) + (width - 1) * (dx == 1)
        return values[at : at + 1]

    def write_notes(target, values):
        total = jnp.sum(values, axis=0, keepdims=True)
        squares = jnp.sum(values * values, axis=0, keepdims=True)
        for dy in (-1, 0, 1):
            for dx in (-1, 0, 1):
                place = (dy + 1) * 3 + dx + 1
                corner = corner_of(values, dy, dx)
                target[place] = jnp.concatenate([total, squares, corner, corner], axis=0)

    def post_notes(source, frame, section_to, sent, receivers):
        for peer in receivers:
            there = lax.rem(peer + shift, tiles)
            dy, dx = there // across - row, lax.rem(there, across) - column
            near = (dy >= -1) & (dy <= 1) & (dx >= -1) & (dx <= 1)
            pltpu.make_async_remote_copy(
                src_ref=source.at[jnp.where(near, (dy + 1) * 3 + dx + 1, 4)],
                dst_ref=notes.at[frame, tile],
                send_sem=sent.at[frame],
                recv_sem=note_sem.at[frame],
                device_id={"section": section_to, "tile": peer},
                device_id_type=mesh_id,
            ).start()

    def side_copies(rows, edges, landing, section_to, sent, received):
        copies = []
        for at, (dy, dx) in enumerate(SIDES):
            source = edges.at[int(dx == 1)]
            if dy:
                start = 0 if dy < 0 else pixels - width
                source = rows.at[start : start + width]
            inside, peer = around[dy, dx]
            copy = pltpu.make_async_remote_copy(
                src_ref=source,
                dst_ref=landing.at[3 - at],
                send_sem=sent.at[at],
                recv_sem=received.at[3 - at],
                device_id={"section": section_to, "tile": peer},
                device_id_type=mesh_id,
            )
            copies.append((inside, copy))
        return copies

    def each(copies, action):
        for inside, copy in copies:
            @pl.when(inside)
            def _():
                action(copy)

    def start(copy):
        copy.start()

    def departed(copy):
        copy.wait_send()

    def arrived(copies):
        for at, (_, copy) in enumerate(copies):
            inside, _ = copies[at // 4 * 4 + 3 - at % 4]

            @pl.when(inside)
            def _():
                copy.wait_recv()

    def old_copies(old):
        copies = side_copies(
            history.at[old], old_columns.at[old], old_sides.at[old], section, old_sent.at[old], old_sem.at[old]
        )
        for at, (dy, dx) in enumerate(CORNERS):
            inside, peer = around[dy, dx]
            copy = pltpu.make_async_remote_copy(
                src_ref=old_drafts.at[old, at],
                dst_ref=old_corners.at[old, 3 - at],
                send_sem=corner_sent.at[old, at],
                recv_sem=corner_sem.at[old, 3 - at],
                device_id={"section": section, "tile": peer},
                device_id_type=mesh_id,
            )
            copies.append((inside, copy))
        return copies

    def first_sides(frame):
        return side_copies(
            main.at[frame], columns.at[count + frame], sides.at[frame], section,
            first_side_sent.at[frame], side_sem.at[frame],
        )

    def next_sides(frame):
        return side_copies(
            outgoing.at[frame], columns.at[frame], sides.at[frame], section + onward.astype(jnp.int32),
            side_sent.at[frame], side_sem.at[frame],
        )

    def own_note(frame):
        return pltpu.make_async_copy(drafts.at[count + frame, 4], notes.at[frame, tile], note_sem.at[frame])

    def open_frame(frame):
        each(first_sides(frame), start)
        post_notes(drafts.at[count + frame], frame, section, first_sent, peers)
        own_note(frame).start()

    def prepare_frame(frame):
        fetch_frame(frame).wait()
        values = main[frame].astype(jnp.float32)
        edge_columns(columns.at[count + frame], values)
        write_notes(drafts.at[count + frame], values)

    @pl.when(first)
    def _():
        prepare_frame(0)

    pl.semaphore_wait(barrier, jnp.where(onward, 2 * tiles - 1, tiles - 1))

    @pl.when(first)
    def _():
        open_frame(0)

    for old in range(context):
        fetch_cache[old].wait()
        values = history[old].astype(jnp.float32)
        edge_columns(old_columns.at[old], values)
        for at, (dy, dx) in enumerate(CORNERS):
            old_drafts[old, at] = corner_of(values, dy, dx)
        each(old_copies(old), start)

    @pl.when(first)
    def _():
        for frame in range(1, count):
            prepare_frame(frame)
            open_frame(frame)

    def lay_out(values, side, corner, act):
        centre = act(values)
        for y in range(height):
            wide[(1 + y) * pitch + EDGE : (1 + y) * pitch + EDGE + width, :] = centre[
                y * width : (y + 1) * width
            ]
        for at, (dy, dx) in enumerate(SIDES):
            inside, _ = around[dy, dx]
            piece = jnp.where(inside, act(side(at).astype(jnp.float32)), 0.0)
            if dy:
                base = (0 if dy < 0 else height + 1) * pitch + EDGE
                wide[base : base + width, :] = piece
            else:
                base = pitch + (EDGE - 1 if dx < 0 else EDGE + width)
                wide[pl.ds(base, height, stride=pitch), :] = piece
        for at, (dy, dx) in enumerate(CORNERS):
            inside, sender = around[dy, dx]
            base = (0 if dy < 0 else height + 1) * pitch + (EDGE - 1 if dx < 0 else EDGE + width)
            wide[base : base + 1, :] = jnp.where(inside, act(corner(at, sender)), 0.0)
        for line in range(height + 2):
            for dx in range(3):
                at = line * pitch + EDGE - 1 + dx
                patches[line * width : (line + 1) * width, dx * channels : (dx + 1) * channels] = wide[
                    at : at + width, :
                ].astype(jnp.bfloat16)

    def convolved(*times):
        rows = jnp.concatenate(
            [patches[dy * width : dy * width + pixels, :] for dy in range(3)], axis=1
        )
        depth = 9 * channels
        kernels = [weight[t * depth : (t + 1) * depth, :] for t in times]
        kernels = kernels[0] if len(kernels) == 1 else jnp.concatenate(kernels, axis=1)
        return jnp.dot(rows, kernels, preferred_element_type=jnp.float32)

    fetch_weight.wait()
    fresh = set()

    def spread(newest, times):
        reach = [t for t in times if 0 <= newest - t < count]
        if reach:
            both = convolved(*reach)
        for at, t in enumerate(reach):
            value = both[:, at * channels : (at + 1) * channels]
            if newest - t in fresh:
                totals[newest - t] += value
            else:
                totals[newest - t] = value
                fresh.add(newest - t)

    for old in range(context):
        arrived(old_copies(old))
        lay_out(
            history[old].astype(jnp.float32),
            lambda at: old_sides[old, at],
            lambda at, sender: old_corners[old, at],
            lambda values: values,
        )
        spread(old, range(taps))

    for fetch in fetch_vectors:
        fetch.wait()
    bias, gain, offset = vectors[0], vectors[1], vectors[2]
    members = pixels * tiles * (channels // GROUPS)
    lane = lax.broadcasted_iota(jnp.int32, (2, channels), 1)

    for frame in range(count):
        pltpu.make_async_copy(notes.at[frame], notes.at[frame], note_sem.at[frame]).wait()
        arrived(next_sides(frame))

        @pl.when(jnp.logical_not(first))
        def _():
            fetch_frame(frame).wait()

        sums = notes[frame, 0, 0:2]
        for sender in range(1, tiles):
            sums = sums + notes[frame, sender, 0:2]
        step = 1
        while step < channels // GROUPS:
            sums = sums + jnp.where(
                (lane // step) % 2 == 0,
                jnp.roll(sums, channels - step, 1),
                jnp.roll(sums, step, 1),
            )
            step *= 2
        mean = sums[0:1] / members
        variance = jnp.maximum(sums[1:2] / members - mean * mean, 0.0)
        scale = gain / jnp.sqrt(variance + EPSILON)

        def act(values):
            value = (values - mean) * scale + offset
            return value / (1.0 + jnp.exp(-value))

        values = main[frame].astype(jnp.float32)
        lay_out(
            values, lambda at: sides[frame, at], lambda at, sender: notes[frame, sender, 2:3], act
        )
        result = values + bias + convolved(taps - 1)
        if frame in fresh:
            result = result + totals[frame]
        rounded = result.astype(jnp.bfloat16)
        out_ref[frame] = rounded

        @pl.when(onward)
        def _():
            outgoing[frame] = rounded
            kept = rounded.astype(jnp.float32)
            write_notes(drafts.at[frame], kept)
            post_notes(drafts.at[frame], frame, section + 1, note_sent, peers + [tile])
            edge_columns(columns.at[frame], kept)
            each(next_sides(frame), start)
            pltpu.make_async_remote_copy(
                src_ref=outgoing.at[frame],
                dst_ref=main.at[frame],
                send_sem=main_sent.at[frame],
                recv_sem=main_sem.at[frame],
                device_id={"section": section + 1, "tile": tile},
                device_id_type=mesh_id,
            ).start()

        spread(context + frame, range(taps - 1))

    for old in range(context):
        each(old_copies(old), departed)

    @pl.when(first)
    def _():
        for frame in range(count):
            each(first_sides(frame), departed)
            some = notes.at[frame, 0 : tiles - 1]
            pltpu.make_async_copy(some, some, first_sent.at[frame]).wait()

    @pl.when(onward)
    def _():
        for frame in range(count):
            pltpu.make_async_copy(outgoing.at[frame], outgoing.at[frame], main_sent.at[frame]).wait()
            pltpu.make_async_copy(notes.at[frame], notes.at[frame], note_sent.at[frame]).wait()
            each(next_sides(frame), departed)


def local(frames, cache, conv_weight, conv_bias, norm_gain, norm_bias):
    sections = lax.axis_size("section")
    tiles = lax.axis_size("tile")
    count, _, height, width, channels = frames.shape
    context = cache.shape[1]
    pixels = height * width
    pitch = width + 2 * EDGE
    rows = conv_weight.size // channels
    vmem = pl.BlockSpec(memory_space=pltpu.VMEM)
    anywhere = pl.BlockSpec(memory_space=pl.ANY)
    dma = pltpu.SemaphoreType.DMA
    half, full = jnp.bfloat16, jnp.float32
    result = pl.pallas_call(
        functools.partial(kernel, sections, tiles, height, width),
        out_shape=pltpu.VMEM((count, pixels, channels), jnp.bfloat16),
        in_specs=[anywhere] * 6,
        out_specs=vmem,
        scratch_shapes=[
            pltpu.VMEM((rows, channels), half),
            pltpu.VMEM((3, 1, channels), full),
            pltpu.VMEM((count, pixels, channels), half),
            pltpu.VMEM((context, pixels, channels), half),
            pltpu.VMEM((count, pixels, channels), half),
            pltpu.VMEM((count, tiles, 4, channels), full),
            pltpu.VMEM((2 * count, 9, 4, channels), full),
            pltpu.VMEM((count, 4, width, channels), half),
            pltpu.VMEM((2 * count, 2, height, channels), half),
            pltpu.VMEM((context, 4, width, channels), half),
            pltpu.VMEM((context, 2, height, channels), half),
            pltpu.VMEM((context, 4, 1, channels), full),
            pltpu.VMEM((context, 4, 1, channels), full),
            pltpu.VMEM((count, pixels, channels), full),
            pltpu.VMEM(((height + 2) * pitch, channels), full),
            pltpu.VMEM(((height + 2) * width, 3 * channels), half),
            pltpu.VMEM((pixels, channels), full),
            dma,
            dma((3,)),
            dma((count,)),
            dma((count,)),
            dma((context,)),
            dma((count,)),
            dma((count,)),
            dma((count,)),
            dma((count, 4)),
            dma((count, 4)),
            dma((count, 4)),
            dma((context, 4)),
            dma((context, 4)),
            dma((context, 4)),
            dma((context, 4)),
        ],
        compiler_params=pltpu.CompilerParams(collective_id=0, has_side_effects=True),
    )(
        frames.reshape(count, pixels, channels),
        cache.reshape(context, pixels, channels),
        conv_weight.reshape(rows, channels),
        conv_bias,
        norm_gain,
        norm_bias,
    )
    return result.reshape(1, count, 1, height, width, channels)


def solution(mesh):
    placed = (
        P("parts", "tile", None, None, None),
        P("section", "parts", "tile", None, None, None),
        P("section", None, None, None, None, None),
        P("section", None),
        P("section", None),
        P("section", None),
    )
    return jax.shard_map(
        local,
        mesh=mesh,
        in_specs=placed,
        out_specs=P("section", "parts", "tile", None, None, None),
        check_vma=False,
    )
```

```python
import functools

import jax
import jax.numpy as jnp
from jax import lax
from jax.experimental import pallas as pl
from jax.experimental.pallas import tpu as pltpu
from jax.sharding import PartitionSpec as P

GROUPS = 32
EPSILON = 1e-06
EDGE = 8


SIDES = ((-1, 0), (0, -1), (0, 1), (1, 0))
CORNERS = ((-1, -1), (-1, 1), (1, -1), (1, 1))


def kernel(
    sections, tiles, height, width,
    frames_hbm, cache_hbm, weight_hbm, bias_hbm, gain_hbm, offset_hbm, out_ref,
    weight, vectors, main, history, outgoing, notes, drafts, sides, columns,
    old_sides, old_columns, old_corners, old_drafts, totals, wide, patches, state,
    weight_sem, vector_sem, main_sem, main_sent, history_sem, note_sem, note_sent, first_sent,
    side_sem, side_sent, first_side_sent, old_sem, old_sent, corner_sem, corner_sent,
):
    count, pixels, channels = main.shape
    context = history.shape[0]
    taps = weight.shape[0] // (9 * channels)
    pitch = width + 2 * EDGE
    section = lax.axis_index("section")
    tile = lax.axis_index("tile")
    across = min(8, tiles // 2)
    down = tiles // across
    shift = across + 2
    mesh_id = pl.DeviceIdType.MESH
    first = section == 0
    onward = section < sections - 1
    image = lax.rem(tile + shift, tiles)
    row, column = image // across, lax.rem(image, across)
    peers = [lax.rem(tile + step, tiles) for step in range(1, tiles)]

    around = {}
    for dy, dx in SIDES + CORNERS:
        y, x = row + dy, column + dx
        inside = (y >= 0) & (y < down) & (x >= 0) & (x < across)
        there = lax.rem(y * across + x + 2 * tiles - shift, tiles)
        around[dy, dx] = inside, jnp.where(inside, there, peers[0])

    barrier = pltpu.get_barrier_semaphore()
    for peer in peers:
        pl.semaphore_signal(
            barrier, inc=1, device_id={"section": section, "tile": peer}, device_id_type=mesh_id
        )

    @pl.when(jnp.logical_not(first))
    def _():
        for peer in peers + [tile]:
            pl.semaphore_signal(
                barrier, inc=1, device_id={"section": section - 1, "tile": peer}, device_id_type=mesh_id
            )

    def fetch_frame(frame):
        return pltpu.make_async_copy(frames_hbm.at[frame], main.at[frame], main_sem.at[frame])

    fetch_weight = pltpu.make_async_copy(weight_hbm, weight, weight_sem)
    fetch_cache = [
        pltpu.make_async_copy(cache_hbm.at[old], history.at[old], history_sem.at[old])
        for old in range(context)
    ]

    @pl.when(first)
    def _():
        for frame in range(count):
            fetch_frame(frame).start()

    fetch_vectors = [
        pltpu.make_async_copy(source, vectors.at[at], vector_sem.at[at])
        for at, source in enumerate((bias_hbm, gain_hbm, offset_hbm))
    ]
    for fetch in fetch_cache + [fetch_weight] + fetch_vectors:
        fetch.start()

    def edge_columns(target, values):
        state[...] = values
        for at, x in enumerate((0, width - 1)):
            target[at] = state[pl.ds(x, height, stride=width), :].astype(jnp.bfloat16)

    def corner_of(values, dy, dx):
        at = (height - 1) * width * (dy == 1) + (width - 1) * (dx == 1)
        return values[at : at + 1]

    def write_notes(target, values):
        total = jnp.sum(values, axis=0, keepdims=True)
        squares = jnp.sum(values * values, axis=0, keepdims=True)
        for dy in (-1, 0, 1):
            for dx in (-1, 0, 1):
                place = (dy + 1) * 3 + dx + 1
                corner = corner_of(values, dy, dx)
                target[place] = jnp.concatenate([total, squares, corner, corner], axis=0)

    def post_notes(source, frame, section_to, sent, receivers):
        for peer in receivers:
            there = lax.rem(peer + shift, tiles)
            dy, dx = there // across - row, lax.rem(there, across) - column
            near = (dy >= -1) & (dy <= 1) & (dx >= -1) & (dx <= 1)
            pltpu.make_async_remote_copy(
                src_ref=source.at[jnp.where(near, (dy + 1) * 3 + dx + 1, 4)],
                dst_ref=notes.at[frame, tile],
                send_sem=sent,
                recv_sem=note_sem.at[frame],
                device_id={"section": section_to, "tile": peer},
                device_id_type=mesh_id,
            ).start()

    def side_copies(rows, edges, landing, section_to, sent, received):
        copies = []
        for at, (dy, dx) in enumerate(SIDES):
            source = edges.at[int(dx == 1)]
            if dy:
                start = 0 if dy < 0 else pixels - width
                source = rows.at[start : start + width]
            inside, peer = around[dy, dx]
            copy = pltpu.make_async_remote_copy(
                src_ref=source,
                dst_ref=landing.at[3 - at],
                send_sem=sent.at[at],
                recv_sem=received.at[3 - at],
                device_id={"section": section_to, "tile": peer},
                device_id_type=mesh_id,
            )
            copies.append((inside, copy))
        return copies

    def each(copies, action):
        for inside, copy in copies:
            @pl.when(inside)
            def _():
                action(copy)

    def start(copy):
        copy.start()

    def arrived(copies):
        for at, (_, copy) in enumerate(copies):
            inside, _ = copies[at // 4 * 4 + 3 - at % 4]

            @pl.when(inside)
            def _():
                copy.wait_recv()

    def old_copies(old):
        copies = side_copies(
            history.at[old], old_columns.at[old], old_sides.at[old], section, old_sent, old_sem.at[old]
        )
        for at, (dy, dx) in enumerate(CORNERS):
            inside, peer = around[dy, dx]
            copy = pltpu.make_async_remote_copy(
                src_ref=old_drafts.at[old, at],
                dst_ref=old_corners.at[old, 3 - at],
                send_sem=corner_sent.at[at],
                recv_sem=corner_sem.at[old, 3 - at],
                device_id={"section": section, "tile": peer},
                device_id_type=mesh_id,
            )
            copies.append((inside, copy))
        return copies

    def first_sides(frame):
        return side_copies(
            main.at[frame], columns.at[count + frame], sides.at[frame], section,
            first_side_sent, side_sem.at[frame],
        )

    def next_sides(frame):
        return side_copies(
            outgoing.at[frame], columns.at[frame], sides.at[frame], section + onward.astype(jnp.int32),
            side_sent, side_sem.at[frame],
        )

    def own_note(frame):
        return pltpu.make_async_copy(drafts.at[count + frame, 4], notes.at[frame, tile], note_sem.at[frame])

    def open_frame(frame):
        each(first_sides(frame), start)
        post_notes(drafts.at[count + frame], frame, section, first_sent, peers)
        own_note(frame).start()

    def prepare_frame(frame):
        fetch_frame(frame).wait()
        values = main[frame].astype(jnp.float32)
        edge_columns(columns.at[count + frame], values)
        write_notes(drafts.at[count + frame], values)

    @pl.when(first)
    def _():
        prepare_frame(0)

    pl.semaphore_wait(barrier, jnp.where(onward, 2 * tiles - 1, tiles - 1))

    @pl.when(first)
    def _():
        open_frame(0)

    for old in range(context):
        fetch_cache[old].wait()
        values = history[old].astype(jnp.float32)
        edge_columns(old_columns.at[old], values)
        for at, (dy, dx) in enumerate(CORNERS):
            old_drafts[old, at] = corner_of(values, dy, dx)
        each(old_copies(old), start)

    @pl.when(first)
    def _():
        for frame in range(1, count):
            prepare_frame(frame)
            open_frame(frame)

    def lay_out(values, side, corner, act):
        centre = act(values)
        for y in range(height):
            wide[(1 + y) * pitch + EDGE : (1 + y) * pitch + EDGE + width, :] = centre[
                y * width : (y + 1) * width
            ]
        for at, (dy, dx) in enumerate(SIDES):
            inside, _ = around[dy, dx]
            piece = jnp.where(inside, act(side(at).astype(jnp.float32)), 0.0)
            if dy:
                base = (0 if dy < 0 else height + 1) * pitch + EDGE
                wide[base : base + width, :] = piece
            else:
                base = pitch + (EDGE - 1 if dx < 0 else EDGE + width)
                wide[pl.ds(base, height, stride=pitch), :] = piece
        for at, (dy, dx) in enumerate(CORNERS):
            inside, sender = around[dy, dx]
            base = (0 if dy < 0 else height + 1) * pitch + (EDGE - 1 if dx < 0 else EDGE + width)
            wide[base : base + 1, :] = jnp.where(inside, act(corner(at, sender)), 0.0)
        for line in range(height + 2):
            for dx in range(3):
                at = line * pitch + EDGE - 1 + dx
                patches[line * width : (line + 1) * width, dx * channels : (dx + 1) * channels] = wide[
                    at : at + width, :
                ].astype(jnp.bfloat16)

    def convolved(*times):
        rows = jnp.concatenate(
            [patches[dy * width : dy * width + pixels, :] for dy in range(3)], axis=1
        )
        depth = 9 * channels
        kernels = [weight[t * depth : (t + 1) * depth, :] for t in times]
        kernels = kernels[0] if len(kernels) == 1 else jnp.concatenate(kernels, axis=1)
        return jnp.dot(rows, kernels, preferred_element_type=jnp.float32)

    fetch_weight.wait()
    fresh = set()

    def spread(newest, times):
        reach = [t for t in times if 0 <= newest - t < count]
        if reach:
            both = convolved(*reach)
        for at, t in enumerate(reach):
            value = both[:, at * channels : (at + 1) * channels]
            if newest - t in fresh:
                totals[newest - t] += value
            else:
                totals[newest - t] = value
                fresh.add(newest - t)

    for old in range(context):
        arrived(old_copies(old))
        lay_out(
            history[old].astype(jnp.float32),
            lambda at: old_sides[old, at],
            lambda at, sender: old_corners[old, at],
            lambda values: values,
        )
        spread(old, range(taps))

    for fetch in fetch_vectors:
        fetch.wait()
    bias, gain, offset = vectors[0], vectors[1], vectors[2]
    members = pixels * tiles * (channels // GROUPS)
    lane = lax.broadcasted_iota(jnp.int32, (2, channels), 1)

    for frame in range(count):
        pltpu.make_async_copy(notes.at[frame], notes.at[frame], note_sem.at[frame]).wait()
        arrived(next_sides(frame))

        @pl.when(jnp.logical_not(first))
        def _():
            fetch_frame(frame).wait()

        sums = notes[frame, 0, 0:2]
        for sender in range(1, tiles):
            sums = sums + notes[frame, sender, 0:2]
        step = 1
        while step < channels // GROUPS:
            sums = sums + jnp.where(
                (lane // step) % 2 == 0,
                jnp.roll(sums, channels - step, 1),
                jnp.roll(sums, step, 1),
            )
            step *= 2
        mean = sums[0:1] / members
        variance = jnp.maximum(sums[1:2] / members - mean * mean, 0.0)
        scale = gain / jnp.sqrt(variance + EPSILON)

        def act(values):
            value = (values - mean) * scale + offset
            return value / (1.0 + jnp.exp(-value))

        values = main[frame].astype(jnp.float32)
        lay_out(
            values, lambda at: sides[frame, at], lambda at, sender: notes[frame, sender, 2:3], act
        )
        result = values + bias + convolved(taps - 1)
        if frame in fresh:
            result = result + totals[frame]
        rounded = result.astype(jnp.bfloat16)
        out_ref[frame] = rounded

        @pl.when(onward)
        def _():
            outgoing[frame] = rounded
            kept = rounded.astype(jnp.float32)
            write_notes(drafts.at[frame], kept)
            post_notes(drafts.at[frame], frame, section + 1, note_sent, peers + [tile])
            edge_columns(columns.at[frame], kept)
            each(next_sides(frame), start)
            pltpu.make_async_remote_copy(
                src_ref=outgoing.at[frame],
                dst_ref=main.at[frame],
                send_sem=main_sent,
                recv_sem=main_sem.at[frame],
                device_id={"section": section + 1, "tile": tile},
                device_id_type=mesh_id,
            ).start()

        spread(context + frame, range(taps - 1))

    def departed(buffer, sent):
        pltpu.make_async_copy(buffer, buffer, sent).wait()

    def sides_departed(buffer, sent, places):
        for at, place in enumerate(places):
            inside, _ = around[place]

            @pl.when(inside)
            def _():
                departed(buffer.at[:, at], sent.at[at])

    sides_departed(old_sides, old_sent, SIDES)
    sides_departed(old_corners, corner_sent, CORNERS)

    @pl.when(first)
    def _():
        departed(notes.at[:, 0 : tiles - 1], first_sent)
        sides_departed(sides, first_side_sent, SIDES)

    @pl.when(onward)
    def _():
        departed(outgoing, main_sent)
        departed(notes, note_sent)
        sides_departed(sides, side_sent, SIDES)


def local(frames, cache, conv_weight, conv_bias, norm_gain, norm_bias):
    sections = lax.axis_size("section")
    tiles = lax.axis_size("tile")
    count, _, height, width, channels = frames.shape
    context = cache.shape[1]
    pixels = height * width
    pitch = width + 2 * EDGE
    rows = conv_weight.size // channels
    vmem = pl.BlockSpec(memory_space=pltpu.VMEM)
    anywhere = pl.BlockSpec(memory_space=pl.ANY)
    dma = pltpu.SemaphoreType.DMA
    half, full = jnp.bfloat16, jnp.float32
    result = pl.pallas_call(
        functools.partial(kernel, sections, tiles, height, width),
        out_shape=pltpu.VMEM((count, pixels, channels), jnp.bfloat16),
        in_specs=[anywhere] * 6,
        out_specs=vmem,
        scratch_shapes=[
            pltpu.VMEM((rows, channels), half),
            pltpu.VMEM((3, 1, channels), full),
            pltpu.VMEM((count, pixels, channels), half),
            pltpu.VMEM((context, pixels, channels), half),
            pltpu.VMEM((count, pixels, channels), half),
            pltpu.VMEM((count, tiles, 4, channels), full),
            pltpu.VMEM((2 * count, 9, 4, channels), full),
            pltpu.VMEM((count, 4, width, channels), half),
            pltpu.VMEM((2 * count, 2, height, channels), half),
            pltpu.VMEM((context, 4, width, channels), half),
            pltpu.VMEM((context, 2, height, channels), half),
            pltpu.VMEM((context, 4, 1, channels), full),
            pltpu.VMEM((context, 4, 1, channels), full),
            pltpu.VMEM((count, pixels, channels), full),
            pltpu.VMEM(((height + 2) * pitch, channels), full),
            pltpu.VMEM(((height + 2) * width, 3 * channels), half),
            pltpu.VMEM((pixels, channels), full),
            dma,
            dma((3,)),
            dma((count,)),
            dma,
            dma((context,)),
            dma((count,)),
            dma,
            dma,
            dma((count, 4)),
            dma((4,)),
            dma((4,)),
            dma((context, 4)),
            dma((4,)),
            dma((context, 4)),
            dma((4,)),
        ],
        compiler_params=pltpu.CompilerParams(collective_id=0, has_side_effects=True),
    )(
        frames.reshape(count, pixels, channels),
        cache.reshape(context, pixels, channels),
        conv_weight.reshape(rows, channels),
        conv_bias,
        norm_gain,
        norm_bias,
    )
    return result.reshape(1, count, 1, height, width, channels)


def solution(mesh):
    placed = (
        P("parts", "tile", None, None, None),
        P("section", "parts", "tile", None, None, None),
        P("section", None, None, None, None, None),
        P("section", None),
        P("section", None),
        P("section", None),
    )
    return jax.shard_map(
        local,
        mesh=mesh,
        in_specs=placed,
        out_specs=P("section", "parts", "tile", None, None, None),
        check_vma=False,
    )
```
